32 devices in a mesh: row: 16 (over z, y, core), col: 2 (over x).
Axes of the slice: x: 2, y: 2, z: 4, core: 2. Of those that a mesh axis runs over, the one named last changes fastest.
Arguments:
- eigvec: float32 [65536, 1024], P('row', 'col'), may hold values from -6 to 6
- reflectors: float32 [16, 2, 1024, 256], P('row', 'col'), may hold values from -0.125 to 0.125
- tfactors: float32 [16, 2, 256, 256], P('row', 'col'), may hold values from -1 to 1, as said below
- offsets: int32 [2, 16], replicated, may hold values from 3072 to 3584
- owners: int32 [2, 16], replicated, may hold values from 0 to 1
Outputs:
- result: float32 [65536, 1024], P('row', 'col')
The draws below stay inside these ranges and needn't reach their ends.
Inputs may be any that keep to these rules, and one draw needn't show every extreme that they name: `tfactors`: every factor block is zero below its diagonal.
All inputs are finite; a program needn't handle non-finite values.
Results may differ from the reference program's by a relative error of at most 0.0003.
Values sent between devices are 32-bit elements; how exact they have to be, the bound alone decides.
A program may use at most 64 MiB of HBM per device.

```python
import jax
import jax.numpy as jnp
from jax import lax

ORDER = 65536
WIN = 1024
BLOCK = 256
TICKS = 2
HALF = 512
ROWS_DEV = 4096
NCOLS = 1024
N_ROW = 16
N_COL = 2


def draw_tfactors(key, part):
    key_diag, key_upper = jax.random.split(jax.random.fold_in(key, 11))
    diagonal = jax.random.uniform(key_diag, (N_ROW, N_COL, BLOCK), jnp.float32, 0.3, 1.0)
    off_scale = 0.6
    entries = jax.random.normal(key_upper, (N_ROW, N_COL, BLOCK, BLOCK), jnp.float32) * (off_scale / BLOCK ** 0.5)
    positions = jnp.arange(BLOCK)
    strict_mask = positions[:, None] < positions[None, :]
    identity = (positions[:, None] == positions[None, :]).astype(jnp.float32)
    return jnp.where(strict_mask, entries, 0.0) + diagonal[..., None] * identity


def plant(result, rng, smallest, top_value):
    longest = result.shape.index(max(result.shape))
    spots = []
    for shift in (0, 1):
        where = [jax.random.randint(jax.random.fold_in(rng, axis), (), 0, length) for axis, length in enumerate(result.shape)]
        where[longest] = (where[longest] + shift) % result.shape[longest]
        spots.append(tuple(where))
    return result.at[spots[0]].set(smallest).at[spots[1]].set(top_value)


def steps_of(own_key, extent, cuts, least, high):
    loudness, own = 1.0, jax.random.fold_in(own_key, 6)
    for dim, parts in cuts:
        draws = jnp.exp(jax.random.uniform(jax.random.fold_in(own, dim), (parts,), jnp.float32, least / len(cuts), high / len(cuts)))
        loudness = loudness * jnp.repeat(draws, extent[dim] // parts).reshape([-1 if axis == dim else 1 for axis in range(len(extent))])
    return loudness


def bell_draw(stream_key, extent, scale, most, cuts=(), kind=jnp.bfloat16):
    level = steps_of(stream_key, extent, cuts, -0.22, 0.18) if cuts else 1.0
    array = jax.random.normal(stream_key, extent, jnp.float32) * scale * level
    return jnp.minimum(jnp.maximum(array, -most), most).astype(kind)


def setup_inputs(seed: int = 0) -> dict:
    key_of = jax.random.split(jax.random.key(seed), 6)
    return {
        "eigvec": bell_draw(key_of[0], (ORDER, NCOLS), 1.0, 6.0, ((0, 16), (1, 2)), jnp.float32),
        "reflectors": bell_draw(key_of[1], (N_ROW, N_COL, WIN, BLOCK), (2 * WIN) ** -0.5, 0.125, ((0, 16), (1, 2)), jnp.float32),
        "tfactors": draw_tfactors(jax.random.fold_in(key_of[5], 71), 0),
        "offsets": plant(jax.random.randint(key_of[3], (TICKS, N_ROW), ROWS_DEV - WIN, ROWS_DEV - HALF + 1), jax.random.fold_in(key_of[3], 1), ROWS_DEV - WIN, ROWS_DEV - HALF).astype(jnp.int32),
        "owners": plant(jax.random.randint(key_of[4], (TICKS, N_ROW), 0, N_COL), jax.random.fold_in(key_of[4], 1), 0, N_COL - 1).astype(jnp.int32),
    }


def project(vectors, window):
    return lax.dot_general(vectors, window, (((0,), (0,)), ((), ())), precision=lax.Precision.HIGHEST, preferred_element_type=jnp.float32)


def reference(eigvec, reflectors, tfactors, offsets, owners):
    row_count = ORDER // N_ROW
    half_rows = WIN // 2
    matrix = jnp.concatenate([eigvec, jnp.zeros((half_rows, eigvec.shape[1]), eigvec.dtype)], 0)
    for turn_index in range(TICKS):
        def update_slab(matrix, slab_index):
            begin_row = (slab_index * row_count + offsets[turn_index, slab_index]).astype(jnp.int32)
            source = owners[turn_index, slab_index]
            vector_block = reflectors[slab_index, source]
            factor_block = tfactors[slab_index, source]
            window = lax.dynamic_slice_in_dim(matrix, begin_row, WIN, 0)
            coefficients = project(vector_block, window)
            scaled = jnp.dot(factor_block, coefficients, precision=lax.Precision.HIGHEST, preferred_element_type=jnp.float32)
            window = window - jnp.dot(vector_block, scaled, precision=lax.Precision.HIGHEST, preferred_element_type=jnp.float32)
            return lax.dynamic_update_slice_in_dim(matrix, window, begin_row, 0), None

        matrix, unused = lax.scan(update_slab, matrix, jnp.arange(N_ROW, dtype=jnp.int32))
    return matrix[:ORDER]
```

```python
import functools

import jax
import jax.numpy as jnp
from jax import lax
from jax.experimental import pallas as pl
from jax.experimental.pallas import tpu as pltpu
from jax.sharding import PartitionSpec as P

WIN = 1024
TICKS = 2
CHUNK = 256
PAD = 8
SUB = 8
LARGE = 56
FUSED = 55


def from_root(block, axis, owner):
    block = jnp.where(lax.axis_index(axis) == owner, block, jnp.zeros_like(block))
    return lax.psum(block, axis)


def from_behind(shard, axis, by):
    count = lax.axis_size(axis)
    pairs = [(i, i + by) for i in range(count) if 0 <= i + by < count]
    return lax.ppermute(shard, axis, pairs)


def positions(n):
    return lax.broadcasted_iota(jnp.int32, (n, n), 0), lax.broadcasted_iota(jnp.int32, (n, n), 1)


def fold(factor):
    half = factor.shape[0] // 2
    r, c = positions(half)
    first, side, second = factor[:half, :half], factor[:half, half:], factor[half:, half:]
    both = jnp.where(r <= c, first, second.T)
    diagonal = jnp.sum(jnp.where(r == c, second, 0.0), axis=0, keepdims=True)
    tail = jnp.pad(diagonal, ((0, PAD - 1), (0, half)))
    return jnp.concatenate([jnp.concatenate([both, side], 1), tail], 0)


def unfold(packed):
    half = packed.shape[1] // 2
    r, c = positions(half)
    both, side, diagonal = packed[:half, :half], packed[:half, half:], packed[half : half + 1, :half]
    first = jnp.where(r <= c, both, 0.0)
    second = jnp.where(r < c, both.T, jnp.where(r == c, jnp.broadcast_to(diagonal, both.shape), 0.0))
    return jnp.concatenate(
        [jnp.concatenate([first, side], 1), jnp.concatenate([jnp.zeros_like(first), second], 1)], 0
    )


def split(x):
    high = x.astype(jnp.bfloat16)
    return high, (x - high.astype(jnp.float32)).astype(jnp.bfloat16)


def product(left, right):
    (lh, ll), (rh, rl) = left, right
    return jnp.dot(
        jnp.concatenate([lh, lh, ll], 1),
        jnp.concatenate([rh, rl, rh], 0),
        preferred_element_type=jnp.float32,
    )


def tiles(x):
    return x.reshape(x.shape[0] // SUB, SUB, x.shape[1])


def rows_from(x, shift):
    turned = pltpu.roll(tiles(x), lax.rem(SUB - shift, SUB), axis=1)
    place = lax.broadcasted_iota(jnp.int32, turned[1:].shape, 1)
    return jnp.where(place + shift < SUB, turned[:-1], turned[1:]).reshape(x.shape[0] - SUB, x.shape[1])


def rows_at(x, shift):
    turned = pltpu.roll(tiles(x), shift, axis=1)
    none = jnp.zeros_like(turned[:1])
    ahead, behind = jnp.concatenate([turned, none], 0), jnp.concatenate([none, turned], 0)
    place = lax.broadcasted_iota(jnp.int32, ahead.shape, 1)
    return jnp.where(place >= shift, ahead, behind).reshape(x.shape[0] + SUB, x.shape[1])


def copy_kernel(width, x_ref, held, head, *uppers):
    step = x_ref.shape[0]
    at = pl.program_id(0)
    first = pl.num_programs(0) - WIN // step
    held[...] = x_ref[...]

    @pl.when(at == 0)
    def _():
        head[...] = x_ref[...]

    for part in range(WIN // step):

        @pl.when(at == first + part)
        def _():
            for chunk, upper in enumerate(uppers):
                upper[part * step : (part + 1) * step, :] = x_ref[:, chunk * width : (chunk + 1) * width]


def cost(flops, values):
    return pl.CostEstimate(flops=flops, bytes_accessed=4 * values, transcendentals=0)


def grant(mib):
    return pltpu.CompilerParams(vmem_limit_bytes=mib * 2**20)


def whole(shape):
    return pl.BlockSpec(shape, lambda i: (0,) * len(shape))


def copy_slab(eigvec, half, width):
    rows, cols = eigvec.shape
    count = cols // width
    rolling = pl.BlockSpec((half, cols), lambda i: (i, 0))
    return pl.pallas_call(
        functools.partial(copy_kernel, width),
        grid=(rows // half,),
        in_specs=[rolling],
        out_specs=[rolling, whole((half, cols))] + [whole((WIN, width))] * count,
        out_shape=[jax.ShapeDtypeStruct(eigvec.shape, jnp.float32), jax.ShapeDtypeStruct((half, cols), jnp.float32)]
        + [jax.ShapeDtypeStruct((WIN, width), jnp.float32)] * count,
        cost_estimate=cost(0, (2 * rows + half + WIN) * cols),
        compiler_params=grant(LARGE),
    )(eigvec)


def window_kernel(plan, va, vb, ta, tb, upper, lower, up_out, low_out, frame):
    end = WIN + lower.shape[0]
    frame[:WIN, :] = upper[...]
    frame[WIN:end, :] = lower[...]
    frame[end:, :] = jnp.zeros_like(frame[end:, :])
    for tick in range(TICKS):
        begin, second = plan[0, tick], plan[1, tick] > 0
        block = jnp.where(second, vb[...], va[...])
        vectors = split(block)
        factor = split(unfold(jnp.where(second, tb[...], ta[...])))
        shift = lax.rem(begin, SUB)
        near = pl.ds(pl.multiple_of(begin - shift, SUB), WIN + SUB)
        window = rows_from(frame[near, :], shift)
        coefficients = product(split(block.T), split(window))
        scaled = product(factor, split(coefficients))
        frame[near, :] -= rows_at(product(vectors, split(scaled)), shift)
    up_out[...] = frame[:WIN, :]
    low_out[...] = frame[WIN:end, :]


def apply_window(plan, va, vb, ta, tb, upper, lower, chunk):
    width = upper.shape[1]
    low = lower.shape[0]
    block = va.shape[1]
    return pl.pallas_call(
        window_kernel,
        grid=(1,),
        in_specs=[pl.BlockSpec(memory_space=pltpu.SMEM)] + [whole(x.shape) for x in (va, vb, ta, tb, upper)]
        + [pl.BlockSpec((low, width), lambda i: (0, chunk))],
        out_specs=[whole((WIN, width)), whole((low, width))],
        out_shape=[
            jax.ShapeDtypeStruct((WIN, width), jnp.float32),
            jax.ShapeDtypeStruct((low, width), jnp.float32),
        ],
        scratch_shapes=[pltpu.VMEM((WIN + low + SUB, width), jnp.float32)],
        cost_estimate=cost(3 * TICKS * 2 * width * block * (2 * WIN + block), 2 * WIN * block + 4 * WIN * width),
        compiler_params=grant(60),
    )(plan, va, vb, ta, tb, upper, lower)


def store_kernel(*refs):
    *parts, held, out = refs
    for chunk, part in enumerate(parts):
        width = part.shape[1]
        out[:, chunk * width : (chunk + 1) * width] = part[...]


def store_upper(parts, held):
    rows, cols = held.shape
    return pl.pallas_call(
        store_kernel,
        grid=(1,),
        in_specs=[whole(part.shape) for part in parts] + [pl.BlockSpec(memory_space=pltpu.HBM)],
        out_specs=pl.BlockSpec((WIN, cols), lambda i: (rows // WIN - 1, 0)),
        out_shape=jax.ShapeDtypeStruct(held.shape, jnp.float32),
        input_output_aliases={len(parts): 0},
        cost_estimate=cost(0, 2 * WIN * cols),
        compiler_params=grant(12),
    )(*parts, held)


def top_kernel(first, top, head, held, out):
    out[...] = jnp.where(first[0] > 0, head[...], top[...])


def store_top(first, top, head, held, chunk):
    half, width = top.shape
    return pl.pallas_call(
        top_kernel,
        grid=(1,),
        in_specs=[
            pl.BlockSpec(memory_space=pltpu.SMEM),
            whole(top.shape),
            pl.BlockSpec((half, width), lambda i: (0, chunk)),
            pl.BlockSpec(memory_space=pltpu.HBM),
        ],
        out_specs=pl.BlockSpec((half, width), lambda i: (0, chunk)),
        out_shape=jax.ShapeDtypeStruct(held.shape, jnp.float32),
        input_output_aliases={3: 0},
        cost_estimate=cost(0, 3 * half * width),
        compiler_params=grant(4),
    )(first, top, head, held)


PIECES = 4
PART = 256
MESH = pl.DeviceIdType.MESH


def triple(left, right):
    (lh, ll), (rh, rl) = left, right
    return jnp.dot(
        jnp.concatenate([lh, lh, ll], 1),
        jnp.concatenate([rh, rl, rh], 0),
        preferred_element_type=jnp.float32,
    )


def shifted(ref, start, count, cols):
    tile = lax.div(start, SUB)
    return rows_from(ref[pl.ds(tile * SUB, count + SUB), cols], start - tile * SUB)


def fused_kernel(
    x, v, t, offsets, owners, out,
    frame, v_own, v_far, t_own, t_out, t_far, vh, vl, vth, vtl, th, tl, wh, wl, later, p0, u0, u1, low,
    near_sem, v_sent, v_got, t_sent, t_got, low_sent, low_got, back_sent, back_got,
):
    rows, cols = x.shape
    half, block = WIN // 2, v.shape[3]
    quarter = block // 2
    base = rows - WIN
    row, col = lax.axis_index("row"), lax.axis_index("col")
    last = lax.axis_size("row") - 1
    has_above, has_below = row > 0, row < last
    other = {"col": 1 - col}
    parts = [slice(c, c + PART) for c in range(0, cols, PART)]
    step = WIN // PIECES

    def local(src, dst, which):
        return pltpu.make_async_copy(src, dst, near_sem.at[which])

    def remote(src, dst, sent, got, target):
        return pltpu.make_async_remote_copy(
            src_ref=src, dst_ref=dst, send_sem=sent, recv_sem=got, device_id=target, device_id_type=MESH
        )

    load_t = local(t.at[0, 0], t_own, 0)
    load_v = local(v.at[0, 0], v_own, 1)
    load_upper = local(x.at[pl.ds(base, WIN)], frame.at[pl.ds(0, WIN)], 2)
    load_middle = local(x.at[pl.ds(half, base - half)], out.at[pl.ds(half, base - half)], 3)
    load_head = local(x.at[pl.ds(0, half)], out.at[pl.ds(0, half)], 4)
    send_v = [
        remote(v.at[0, 0, pl.ds(k * step, step)], v_far.at[pl.ds(k * step, step)], v_sent.at[k], v_got.at[k], other)
        for k in range(PIECES)
    ]
    send_t = remote(t_out, t_far, t_sent, t_got, other)
    send_low = remote(x.at[pl.ds(0, half)], frame.at[pl.ds(WIN, half)], low_sent, low_got, {"row": row - 1})
    send_back = [
        remote(low.at[:, pl.ds(c * PART, PART)], out.at[pl.ds(0, half), pl.ds(c * PART, PART)],
               back_sent.at[c], back_got.at[c], {"row": row + 1})
        for c in range(len(parts))
    ]

    load_t.start()
    barrier = pltpu.get_barrier_semaphore()
    pl.semaphore_signal(barrier, inc=1, device_id=other, device_id_type=MESH)

    @pl.when(has_above)
    def _():
        pl.semaphore_signal(barrier, inc=1, device_id={"row": row - 1}, device_id_type=MESH)

    @pl.when(has_below)
    def _():
        pl.semaphore_signal(barrier, inc=1, device_id={"row": row + 1}, device_id_type=MESH)

    load_v.start()
    load_upper.start()

    @pl.when(has_above & has_below)
    def _():
        pl.semaphore_wait(barrier, 3)

    @pl.when(jnp.logical_not(has_above & has_below))
    def _():
        pl.semaphore_wait(barrier, 2)

    send_v[0].start()

    @pl.when(has_above)
    def _():
        send_low.start()

    load_middle.start()

    @pl.when(jnp.logical_not(has_above))
    def _():
        load_head.start()

    load_t.wait()
    factor = t_own[...]
    r, c = positions(quarter)
    first, second = factor[:quarter, :quarter], factor[quarter:, quarter:]
    diagonal = jnp.sum(jnp.where(r == c, second, 0.0), axis=0, keepdims=True)
    t_out[:quarter, :quarter] = jnp.where(r <= c, first, second.T)
    t_out[:quarter, quarter:] = factor[:quarter, quarter:]
    t_out[quarter:, :] = jnp.broadcast_to(jnp.concatenate([diagonal, diagonal], 1), (PAD, block))
    th[0], tl[0] = split(factor)
    send_t.start()
    for k in range(1, PIECES):
        send_v[k].start()

    def prepare(source, holder, k):
        span = slice(k * step, (k + 1) * step)
        piece = source[span, :]
        vh[holder, span, :], vl[holder, span, :] = split(piece)
        vth[holder, :, span], vtl[holder, :, span] = split(piece.T)

    load_v.wait()
    for k in range(PIECES):
        prepare(v_own, 0, k)

    begin = [jnp.clip(offsets[tick, row] - base, 0, half) for tick in range(TICKS)]
    holder = [(owners[tick, row] != col).astype(jnp.int32) for tick in range(TICKS)]
    for u in (u0, u1):
        u[:half, :] = jnp.zeros((half, cols), jnp.float32)
        u[half + WIN :, :] = jnp.zeros((half + SUB, cols), jnp.float32)
    frame[WIN + half :, :] = jnp.zeros((SUB, cols), jnp.float32)

    @pl.when(jnp.logical_not(has_below))
    def _():
        frame[WIN : WIN + half, :] = jnp.zeros((half, cols), jnp.float32)

    load_upper.wait()

    @pl.when(has_below)
    def _():
        send_low.wait_recv()

    def windows(k, carry):
        span = pl.ds(pl.multiple_of(k * 128, 128), 128)
        wh[span, :], wl[span, :] = split(shifted(frame, begin[0] + k * 128, 128, slice(None)))
        later[span, :] = shifted(frame, begin[1] + k * 128, 128, slice(None))
        return carry

    lax.fori_loop(0, WIN // 128, windows, 0)

    send_t.wait_recv()
    th[1], tl[1] = split(unfold(t_far[...]))

    for k in range(PIECES):
        send_v[k].wait_recv()
        prepare(v_far, 1, k)
        span = slice(k * step, (k + 1) * step)
        left = vth[holder[0], :, span], vtl[holder[0], :, span]
        for part in parts:
            sums = triple(left, (wh[span, part], wl[span, part]))
            p0[:, part] = sums if k == 0 else p0[:, part] + sums

    factors = [(th[holder[tick]], tl[holder[tick]]) for tick in range(TICKS)]
    scaled = []
    for c, part in enumerate(parts):
        first = split(triple(factors[0], split(p0[:, part])))
        u0[half : half + WIN, part] = triple((vh[holder[0]], vl[holder[0]]), first)
        window = later[:, part] - shifted(u0, half + begin[1] - begin[0], WIN, part)
        sums = triple((vth[holder[1]], vtl[holder[1]]), split(window))
        second = split(triple(factors[1], split(sums)))
        scaled.append(second)
        u1[WIN : half + WIN, part] = triple((vh[holder[1], half:, :], vl[holder[1], half:, :]), second)
        low[:, part] = (
            frame[WIN : WIN + half, part]
            - shifted(u0, WIN + half - begin[0], half, part)
            - shifted(u1, WIN + half - begin[1], half, part)
        )

        @pl.when(has_below)
        def _():
            send_back[c].start()

    for c, part in enumerate(parts):
        u1[half:WIN, part] = triple((vh[holder[1], :half, :], vl[holder[1], :half, :]), scaled[c])

        def upper(k, carry):
            span = pl.ds(pl.multiple_of(k * 128, 128), 128)
            out[pl.ds(pl.multiple_of(base + k * 128, 128), 128), part] = (
                frame[span, part]
                - shifted(u0, half - begin[0] + k * 128, 128, part)
                - shifted(u1, half - begin[1] + k * 128, 128, part)
            )
            return carry

        lax.fori_loop(0, WIN // 128, upper, 0)

    load_middle.wait()

    @pl.when(jnp.logical_not(has_above))
    def _():
        load_head.wait()

    send_t.wait_send()
    for k in range(PIECES):
        send_v[k].wait_send()

    @pl.when(has_above)
    def _():
        send_low.wait_send()
        for copy in send_back:
            copy.wait_recv()

    @pl.when(has_below)
    def _():
        for copy in send_back:
            copy.wait_send()


def fused(eigvec, reflectors, tfactors, offsets, owners):
    _, cols = eigvec.shape
    block = reflectors.shape[3]
    half = WIN // 2
    parts = cols // PART
    f32, bf16 = jnp.float32, jnp.bfloat16
    dma = pltpu.SemaphoreType.DMA
    arrays = [pltpu.with_memory_space_constraint(a, pltpu.HBM) for a in (eigvec, reflectors, tfactors)]
    return pl.pallas_call(
        fused_kernel,
        in_specs=[pl.BlockSpec(memory_space=pltpu.HBM)] * 3 + [pl.BlockSpec(memory_space=pltpu.SMEM)] * 2,
        out_specs=pl.BlockSpec(memory_space=pltpu.VMEM),
        out_shape=pltpu.VMEM(eigvec.shape, f32),
        scratch_shapes=[
            pltpu.VMEM((WIN + half + SUB, cols), f32),
            pltpu.VMEM((WIN, block), f32),
            pltpu.VMEM((WIN, block), f32),
            pltpu.VMEM((block, block), f32),
            pltpu.VMEM((block // 2 + PAD, block), f32),
            pltpu.VMEM((block // 2 + PAD, block), f32),
            pltpu.VMEM((2, WIN, block), bf16),
            pltpu.VMEM((2, WIN, block), bf16),
            pltpu.VMEM((2, block, WIN), bf16),
            pltpu.VMEM((2, block, WIN), bf16),
            pltpu.VMEM((2, block, block), bf16),
            pltpu.VMEM((2, block, block), bf16),
            pltpu.VMEM((WIN, cols), bf16),
            pltpu.VMEM((WIN, cols), bf16),
            pltpu.VMEM((WIN, cols), f32),
            pltpu.VMEM((block, cols), f32),
            pltpu.VMEM((2 * WIN + SUB, cols), f32),
            pltpu.VMEM((2 * WIN + SUB, cols), f32),
            pltpu.VMEM((half, cols), f32),
            dma((5,)),
            dma((PIECES,)),
            dma((PIECES,)),
            dma,
            dma,
            dma,
            dma,
            dma((parts,)),
            dma((parts,)),
        ],
        cost_estimate=cost(10**10, 10**7),
        compiler_params=pltpu.CompilerParams(collective_id=0, has_side_effects=True, vmem_limit_bytes=FUSED * 2**20),
    )(*arrays, offsets, owners)


def per_device(eigvec, reflectors, tfactors, offsets, owners):
    rows, cols = eigvec.shape
    half = WIN // 2
    width = min(CHUNK, cols)
    own_row = lax.axis_index("row")
    holders = lax.axis_size("col")
    if holders == 2:
        return fused(eigvec, reflectors, tfactors, offsets, owners)
    vectors, factor = reflectors[0, 0], tfactors[0, 0]
    packed = fold(factor)
    source = lax.dynamic_slice_in_dim(owners, own_row, 1, 1)[:, 0]
    begin = lax.dynamic_slice_in_dim(offsets, own_row, 1, 1)[:, 0] - (rows - WIN)
    va, vb = (from_root(vectors, "col", source[t]) for t in range(TICKS))
    ta, tb = (from_root(packed, "col", source[t]) for t in range(TICKS))
    second = jnp.arange(TICKS, dtype=jnp.int32)
    plan = jnp.stack([begin, second])
    result, head, *uppers = copy_slab(eigvec, half, width)
    lower = from_behind(head, "row", -1)
    parts, tops = [], []
    for chunk, upper in enumerate(uppers):
        part, low = apply_window(plan, va, vb, ta, tb, upper, lower, chunk)
        parts.append(part)
        tops.append(from_behind(low, "row", 1))
    result = store_upper(parts, result)
    first = (own_row == 0).astype(jnp.int32)[None]
    for chunk, top in enumerate(tops):
        result = store_top(first, top, head, result, chunk)
    return result


def solution(mesh):
    return jax.shard_map(
        per_device,
        mesh=mesh,
        in_specs=(
            P("row", "col"),
            P("row", "col", None, None),
            P("row", "col", None, None),
            P(),
            P(),
        ),
        out_specs=P("row", "col"),
        check_vma=False,
    )
```

```python
import functools

import jax
import jax.numpy as jnp
from jax import lax
from jax.experimental import pallas as pl
from jax.experimental.pallas import tpu as pltpu
from jax.sharding import PartitionSpec as P

WIN = 1024
TICKS = 2
CHUNK = 256
PAD = 8
SUB = 8
LARGE = 56
FUSED = 55


def from_root(block, axis, owner):
    block = jnp.where(lax.axis_index(axis) == owner, block, jnp.zeros_like(block))
    return lax.psum(block, axis)


def from_behind(shard, axis, by):
    count = lax.axis_size(axis)
    pairs = [(i, i + by) for i in range(count) if 0 <= i + by < count]
    return lax.ppermute(shard, axis, pairs)


def positions(n):
    return lax.broadcasted_iota(jnp.int32, (n, n), 0), lax.broadcasted_iota(jnp.int32, (n, n), 1)


def fold(factor):
    half = factor.shape[0] // 2
    r, c = positions(half)
    first, side, second = factor[:half, :half], factor[:half, half:], factor[half:, half:]
    both = jnp.where(r <= c, first, second.T)
    diagonal = jnp.sum(jnp.where(r == c, second, 0.0), axis=0, keepdims=True)
    tail = jnp.pad(diagonal, ((0, PAD - 1), (0, half)))
    return jnp.concatenate([jnp.concatenate([both, side], 1), tail], 0)


def unfold(packed):
    half = packed.shape[1] // 2
    r, c = positions(half)
    both, side, diagonal = packed[:half, :half], packed[:half, half:], packed[half : half + 1, :half]
    first = jnp.where(r <= c, both, 0.0)
    second = jnp.where(r < c, both.T, jnp.where(r == c, jnp.broadcast_to(diagonal, both.shape), 0.0))
    return jnp.concatenate(
        [jnp.concatenate([first, side], 1), jnp.concatenate([jnp.zeros_like(first), second], 1)], 0
    )


def split(x):
    high = x.astype(jnp.bfloat16)
    return high, (x - high.astype(jnp.float32)).astype(jnp.bfloat16)


def product(left, right):
    (lh, ll), (rh, rl) = left, right
    return jnp.dot(
        jnp.concatenate([lh, lh, ll], 1),
        jnp.concatenate([rh, rl, rh], 0),
        preferred_element_type=jnp.float32,
    )


def tiles(x):
    return x.reshape(x.shape[0] // SUB, SUB, x.shape[1])


def rows_from(x, shift):
    turned = pltpu.roll(tiles(x), lax.rem(SUB - shift, SUB), axis=1)
    place = lax.broadcasted_iota(jnp.int32, turned[1:].shape, 1)
    return jnp.where(place + shift < SUB, turned[:-1], turned[1:]).reshape(x.shape[0] - SUB, x.shape[1])


def rows_at(x, shift):
    turned = pltpu.roll(tiles(x), shift, axis=1)
    none = jnp.zeros_like(turned[:1])
    ahead, behind = jnp.concatenate([turned, none], 0), jnp.concatenate([none, turned], 0)
    place = lax.broadcasted_iota(jnp.int32, ahead.shape, 1)
    return jnp.where(place >= shift, ahead, behind).reshape(x.shape[0] + SUB, x.shape[1])


def copy_kernel(width, x_ref, held, head, *uppers):
    step = x_ref.shape[0]
    at = pl.program_id(0)
    first = pl.num_programs(0) - WIN // step
    held[...] = x_ref[...]

    @pl.when(at == 0)
    def _():
        head[...] = x_ref[...]

    for part in range(WIN // step):

        @pl.when(at == first + part)
        def _():
            for chunk, upper in enumerate(uppers):
                upper[part * step : (part + 1) * step, :] = x_ref[:, chunk * width : (chunk + 1) * width]


def cost(flops, values):
    return pl.CostEstimate(flops=flops, bytes_accessed=4 * values, transcendentals=0)


def grant(mib):
    return pltpu.CompilerParams(vmem_limit_bytes=mib * 2**20)


def whole(shape):
    return pl.BlockSpec(shape, lambda i: (0,) * len(shape))


def copy_slab(eigvec, half, width):
    rows, cols = eigvec.shape
    count = cols // width
    rolling = pl.BlockSpec((half, cols), lambda i: (i, 0))
    return pl.pallas_call(
        functools.partial(copy_kernel, width),
        grid=(rows // half,),
        in_specs=[rolling],
        out_specs=[rolling, whole((half, cols))] + [whole((WIN, width))] * count,
        out_shape=[jax.ShapeDtypeStruct(eigvec.shape, jnp.float32), jax.ShapeDtypeStruct((half, cols), jnp.float32)]
        + [jax.ShapeDtypeStruct((WIN, width), jnp.float32)] * count,
        cost_estimate=cost(0, (2 * rows + half + WIN) * cols),
        compiler_params=grant(LARGE),
    )(eigvec)


def window_kernel(plan, va, vb, ta, tb, upper, lower, up_out, low_out, frame):
    end = WIN + lower.shape[0]
    frame[:WIN, :] = upper[...]
    frame[WIN:end, :] = lower[...]
    frame[end:, :] = jnp.zeros_like(frame[end:, :])
    for tick in range(TICKS):
        begin, second = plan[0, tick], plan[1, tick] > 0
        block = jnp.where(second, vb[...], va[...])
        vectors = split(block)
        factor = split(unfold(jnp.where(second, tb[...], ta[...])))
        shift = lax.rem(begin, SUB)
        near = pl.ds(pl.multiple_of(begin - shift, SUB), WIN + SUB)
        window = rows_from(frame[near, :], shift)
        coefficients = product(split(block.T), split(window))
        scaled = product(factor, split(coefficients))
        frame[near, :] -= rows_at(product(vectors, split(scaled)), shift)
    up_out[...] = frame[:WIN, :]
    low_out[...] = frame[WIN:end, :]


def apply_window(plan, va, vb, ta, tb, upper, lower, chunk):
    width = upper.shape[1]
    low = lower.shape[0]
    block = va.shape[1]
    return pl.pallas_call(
        window_kernel,
        grid=(1,),
        in_specs=[pl.BlockSpec(memory_space=pltpu.SMEM)] + [whole(x.shape) for x in (va, vb, ta, tb, upper)]
        + [pl.BlockSpec((low, width), lambda i: (0, chunk))],
        out_specs=[whole((WIN, width)), whole((low, width))],
        out_shape=[
            jax.ShapeDtypeStruct((WIN, width), jnp.float32),
            jax.ShapeDtypeStruct((low, width), jnp.float32),
        ],
        scratch_shapes=[pltpu.VMEM((WIN + low + SUB, width), jnp.float32)],
        cost_estimate=cost(3 * TICKS * 2 * width * block * (2 * WIN + block), 2 * WIN * block + 4 * WIN * width),
        compiler_params=grant(60),
    )(plan, va, vb, ta, tb, upper, lower)


def store_kernel(*refs):
    *parts, held, out = refs
    for chunk, part in enumerate(parts):
        width = part.shape[1]
        out[:, chunk * width : (chunk + 1) * width] = part[...]


def store_upper(parts, held):
    rows, cols = held.shape
    return pl.pallas_call(
        store_kernel,
        grid=(1,),
        in_specs=[whole(part.shape) for part in parts] + [pl.BlockSpec(memory_space=pltpu.HBM)],
        out_specs=pl.BlockSpec((WIN, cols), lambda i: (rows // WIN - 1, 0)),
        out_shape=jax.ShapeDtypeStruct(held.shape, jnp.float32),
        input_output_aliases={len(parts): 0},
        cost_estimate=cost(0, 2 * WIN * cols),
        compiler_params=grant(12),
    )(*parts, held)


def top_kernel(first, top, head, held, out):
    out[...] = jnp.where(first[0] > 0, head[...], top[...])


def store_top(first, top, head, held, chunk):
    half, width = top.shape
    return pl.pallas_call(
        top_kernel,
        grid=(1,),
        in_specs=[
            pl.BlockSpec(memory_space=pltpu.SMEM),
            whole(top.shape),
            pl.BlockSpec((half, width), lambda i: (0, chunk)),
            pl.BlockSpec(memory_space=pltpu.HBM),
        ],
        out_specs=pl.BlockSpec((half, width), lambda i: (0, chunk)),
        out_shape=jax.ShapeDtypeStruct(held.shape, jnp.float32),
        input_output_aliases={3: 0},
        cost_estimate=cost(0, 3 * half * width),
        compiler_params=grant(4),
    )(first, top, head, held)


PIECE = 64
PART = 256
MESH = pl.DeviceIdType.MESH


def triple(left, right):
    (lh, ll), (rh, rl) = left, right
    return jnp.dot(
        jnp.concatenate([lh, lh, ll], 1),
        jnp.concatenate([rh, rl, rh], 0),
        preferred_element_type=jnp.float32,
    )


def shifted(ref, start, count, cols):
    tile = lax.div(start, SUB)
    return rows_from(ref[pl.ds(tile * SUB, count + SUB), cols], start - tile * SUB)


def fused_kernel(
    x, v, t, offsets, owners, out,
    frame, vectors, t_own, t_out, t_far, vt_out, vt_far, vh, vl, vth, vtl, th, tl, wh, wl, p, c, u0, u1,
    above, ah, al, ac, n0, n1,
    near_sem, x_sent, x_got, low_sent, low_got, y_sent, y_got,
):
    rows, cols = x.shape
    half, block = WIN // 2, v.shape[3]
    quarter = block // 2
    base = rows - WIN
    row, col = lax.axis_index("row"), lax.axis_index("col")
    last = lax.axis_size("row") - 1
    has_above, has_below = row > 0, row < last
    other, below = {"col": 1 - col}, {"row": row + 1}
    parts = [slice(at, at + PART) for at in range(0, cols, PART)]
    pieces = [slice(at, at + PIECE) for at in range(block - PIECE, -1, -PIECE)]
    count = len(pieces)
    rests = [(at, half // 2) for at in (0, half // 2)]

    def local(src, dst, which):
        return pltpu.make_async_copy(src, dst, near_sem.at[which])

    def remote(src, dst, sent, got, target):
        return pltpu.make_async_remote_copy(
            src_ref=src, dst_ref=dst, send_sem=sent, recv_sem=got, device_id=target, device_id_type=MESH
        )

    load_t = local(t.at[0, 0], t_own, 0)
    load_v = local(v.at[0, 0], vectors.at[0, pl.ds(half, WIN)], 1)
    load_upper = local(x.at[pl.ds(base, WIN)], frame.at[pl.ds(0, WIN)], 2)
    load_head = local(x.at[pl.ds(0, half)], out.at[pl.ds(0, half)], 3)
    load_middle = local(x.at[pl.ds(half, base - half)], out.at[pl.ds(half, base - half)], 4)
    send_rest = [
        remote(v.at[0, 0, pl.ds(half + at, n)], vectors.at[1, pl.ds(WIN + at, n)], x_sent.at[k], x_got.at[k], other)
        for k, (at, n) in enumerate(rests)
    ]
    send_t = remote(t_out, t_far, x_sent.at[2], x_got.at[2], other)
    send_vt = [
        remote(vt_out.at[pl.ds(piece.start, PIECE)], vt_far.at[pl.ds(piece.start, PIECE)],
               x_sent.at[3 + k], x_got.at[3 + k], other)
        for k, piece in enumerate(pieces)
    ]
    send_low = remote(x.at[pl.ds(0, half)], frame.at[pl.ds(WIN, half)], low_sent, low_got, {"row": row - 1})
    pass_own = remote(v.at[0, 0, pl.ds(half, half)], above.at[0], y_sent.at[0], y_got.at[0], below)
    pass_far = [
        remote(vectors.at[1, pl.ds(WIN + at, n)], above.at[1, pl.ds(at, n)], y_sent.at[1 + k], y_got.at[1 + k], below)
        for k, (at, n) in enumerate(rests)
    ]
    pass_first = [
        remote(c.at[0, pl.ds(piece.start, PIECE)], ac.at[0, pl.ds(piece.start, PIECE)],
               y_sent.at[3 + k], y_got.at[3 + k], below)
        for k, piece in enumerate(pieces)
    ]
    pass_second = [
        remote(c.at[1, :, pl.ds(part.start, PART)], ac.at[1, :, pl.ds(part.start, PART)],
               y_sent.at[3 + count + k], y_got.at[3 + count + k], below)
        for k, part in enumerate(parts)
    ]

    def send_below(copy):
        @pl.when(has_below)
        def _():
            copy.start()

    load_t.start()
    load_v.start()
    barrier = pltpu.get_barrier_semaphore()
    pl.semaphore_signal(barrier, inc=1, device_id=other, device_id_type=MESH)

    @pl.when(has_above)
    def _():
        pl.semaphore_signal(barrier, inc=1, device_id={"row": row - 1}, device_id_type=MESH)

    @pl.when(has_below)
    def _():
        pl.semaphore_signal(barrier, inc=1, device_id=below, device_id_type=MESH)

    load_upper.start()
    load_head.start()

    @pl.when(has_above & has_below)
    def _():
        pl.semaphore_wait(barrier, 3)

    @pl.when(jnp.logical_not(has_above & has_below))
    def _():
        pl.semaphore_wait(barrier, 2)

    for copy in send_rest:
        copy.start()

    @pl.when(has_above)
    def _():
        send_low.start()

    load_middle.start()

    load_t.wait()
    factor = t_own[...]
    r, l = positions(quarter)
    first, second = factor[:quarter, :quarter], factor[quarter:, quarter:]
    diagonal = jnp.sum(jnp.where(r == l, second, 0.0), axis=0, keepdims=True)
    t_out[:quarter, :quarter] = jnp.where(r <= l, first, second.T)
    t_out[:quarter, quarter:] = factor[:quarter, quarter:]
    t_out[quarter:, :] = jnp.broadcast_to(jnp.concatenate([diagonal, diagonal], 1), (PAD, block))
    th[0], tl[0] = split(factor)

    load_v.wait()
    vt_out[...] = vectors[0, half:WIN, :].T
    send_t.start()
    for copy in send_vt:
        copy.start()

    def prepare(which, start, n):
        span = slice(start, start + n)
        piece = vectors[which, half + start : half + start + n, :]
        vh[which, span, :], vl[which, span, :] = split(piece)
        vth[which, :, span], vtl[which, :, span] = split(piece.T)

    for at in range(0, WIN, half // 2):
        prepare(0, at, half // 2)

    begin = [jnp.clip(offsets[tick, row] - base, 0, half) for tick in range(TICKS)]
    holder = [(owners[tick, row] != col).astype(jnp.int32) for tick in range(TICKS)]
    before = jnp.maximum(row - 1, 0)
    above_begin = [jnp.clip(offsets[tick, before] - base, 0, half) for tick in range(TICKS)]
    above_holder = [(owners[tick, before] != col).astype(jnp.int32) for tick in range(TICKS)]
    for u in (u0, u1):
        u[:half, :] = jnp.zeros((half, cols), jnp.float32)
        u[half + WIN :, :] = jnp.zeros((half + SUB, cols), jnp.float32)
    for n in (n0, n1):
        n[half:, :] = jnp.zeros((half + SUB, cols), jnp.float32)
    for which in range(2):
        vectors[which, :half, :] = jnp.zeros((half, block), jnp.float32)
        vectors[which, half + WIN :, :] = jnp.zeros((half + SUB, block), jnp.float32)
    frame[WIN + half :, :] = jnp.zeros((SUB, cols), jnp.float32)
    p[0] = jnp.zeros((block, cols), jnp.float32)

    @pl.when(jnp.logical_not(has_below))
    def _():
        frame[WIN : WIN + half, :] = jnp.zeros((half, cols), jnp.float32)

    load_upper.wait()

    @pl.when(has_below)
    def _():
        send_low.wait_recv()
        pass_own.start()

    for k, (at, n) in enumerate(rests):
        send_rest[k].wait_recv()
        send_below(pass_far[k])
        prepare(1, half + at, n)

    def windows(k, carry):
        span = pl.ds(pl.multiple_of(k * 128, 128), 128)
        for tick in range(TICKS):
            wh[tick, span, :], wl[tick, span, :] = split(shifted(frame, begin[tick] + k * 128, 128, slice(None)))
        return carry

    lax.fori_loop(0, WIN // 128, windows, 0)

    send_t.wait_recv()
    th[1], tl[1] = split(unfold(t_far[...]))

    for k, piece in enumerate(pieces):
        send_vt[k].wait_recv()
        vth[1, piece, :half], vtl[1, piece, :half] = split(vt_far[piece, :])
        for tick in range(TICKS):
            left = vth[holder[tick], piece, :], vtl[holder[tick], piece, :]
            for part in parts:
                p[tick, piece, part] = triple(left, (wh[tick, :, part], wl[tick, :, part]))
            if tick == 0:
                left = th[holder[0], piece, :], tl[holder[0], piece, :]
                for part in parts:
                    c[0, piece, part] = triple(left, split(p[0, :, part]))
                send_below(pass_first[k])
        if piece.start % quarter == 0:
            span = slice(piece.start, piece.start + quarter)
            natural = vt_far[span, :].T
            vectors[1, half:WIN, span] = natural
            vh[1, :half, span], vl[1, :half, span] = split(natural)
        if k == 0:

            @pl.when(has_above)
            def _():
                pass_own.wait_recv()
                for copy in pass_far:
                    copy.wait_recv()
                for which in range(2):
                    ah[which], al[which] = split(above[which])

    moved = split(shifted(vectors.at[holder[0]], half + begin[1] - begin[0], WIN, slice(None)))
    cross = split(triple((vth[holder[1]], vtl[holder[1]]), moved))
    factor = th[holder[1]], tl[holder[1]]
    for k, part in enumerate(parts):
        sums = p[1, :, part] - triple(cross, split(c[0, :, part]))
        c[1, :, part] = triple(factor, split(sums))
        send_below(pass_second[k])

    @pl.when(has_above)
    def _():
        for copy in pass_first:
            copy.wait_recv()
        for part in parts:
            n0[:half, part] = triple((ah[above_holder[0]], al[above_holder[0]]), split(ac[0, :, part]))

    load_head.wait()

    for part in parts:
        for tick, u in enumerate((u0, u1)):
            u[half : half + WIN, part] = triple((vh[holder[tick]], vl[holder[tick]]), split(c[tick, :, part]))

        def upper(k, carry):
            span = pl.ds(pl.multiple_of(k * 128, 128), 128)
            out[pl.ds(pl.multiple_of(base + k * 128, 128), 128), part] = (
                frame[span, part]
                - shifted(u0, half - begin[0] + k * 128, 128, part)
                - shifted(u1, half - begin[1] + k * 128, 128, part)
            )
            return carry

        lax.fori_loop(0, WIN // 128, upper, 0)

    load_middle.wait()
    for copy in (*send_rest, send_t, *send_vt):
        copy.wait_send()

    @pl.when(has_above)
    def _():
        for k, part in enumerate(parts):
            pass_second[k].wait_recv()
            n1[:half, part] = triple((ah[above_holder[1]], al[above_holder[1]]), split(ac[1, :, part]))
            out[:half, part] -= shifted(n0, half - above_begin[0], half, part) + shifted(
                n1, half - above_begin[1], half, part
            )
        send_low.wait_send()

    @pl.when(has_below)
    def _():
        for copy in (pass_own, *pass_far, *pass_first, *pass_second):
            copy.wait_send()


def fused(eigvec, reflectors, tfactors, offsets, owners):
    _, cols = eigvec.shape
    block = reflectors.shape[3]
    half = WIN // 2
    count = block // PIECE
    f32, bf16 = jnp.float32, jnp.bfloat16
    dma = pltpu.SemaphoreType.DMA
    arrays = [pltpu.with_memory_space_constraint(a, pltpu.HBM) for a in (eigvec, reflectors, tfactors)]
    return pl.pallas_call(
        fused_kernel,
        in_specs=[pl.BlockSpec(memory_space=pltpu.HBM)] * 3 + [pl.BlockSpec(memory_space=pltpu.SMEM)] * 2,
        out_specs=pl.BlockSpec(memory_space=pltpu.VMEM),
        out_shape=pltpu.VMEM(eigvec.shape, f32),
        scratch_shapes=[
            pltpu.VMEM((WIN + half + SUB, cols), f32),
            pltpu.VMEM((2, 2 * WIN + SUB, block), f32),
            pltpu.VMEM((block, block), f32),
            pltpu.VMEM((block // 2 + PAD, block), f32),
            pltpu.VMEM((block // 2 + PAD, block), f32),
            pltpu.VMEM((block, half), f32),
            pltpu.VMEM((block, half), f32),
            pltpu.VMEM((2, WIN, block), bf16),
            pltpu.VMEM((2, WIN, block), bf16),
            pltpu.VMEM((2, block, WIN), bf16),
            pltpu.VMEM((2, block, WIN), bf16),
            pltpu.VMEM((2, block, block), bf16),
            pltpu.VMEM((2, block, block), bf16),
            pltpu.VMEM((TICKS, WIN, cols), bf16),
            pltpu.VMEM((TICKS, WIN, cols), bf16),
            pltpu.VMEM((TICKS, block, cols), f32),
            pltpu.VMEM((TICKS, block, cols), f32),
            pltpu.VMEM((2 * WIN + SUB, cols), f32),
            pltpu.VMEM((2 * WIN + SUB, cols), f32),
            pltpu.VMEM((2, half, block), f32),
            pltpu.VMEM((2, half, block), bf16),
            pltpu.VMEM((2, half, block), bf16),
            pltpu.VMEM((TICKS, block, cols), f32),
            pltpu.VMEM((WIN + SUB, cols), f32),
            pltpu.VMEM((WIN + SUB, cols), f32),
            dma((5,)),
            dma((3 + count,)),
            dma((3 + count,)),
            dma,
            dma,
            dma((3 + count + cols // PART,)),
            dma((3 + count + cols // PART,)),
        ],
        cost_estimate=cost(10**10, 10**7),
        compiler_params=pltpu.CompilerParams(collective_id=0, has_side_effects=True, vmem_limit_bytes=FUSED * 2**20),
    )(*arrays, offsets, owners)


def per_device(eigvec, reflectors, tfactors, offsets, owners):
    rows, cols = eigvec.shape
    half = WIN // 2
    width = min(CHUNK, cols)
    own_row = lax.axis_index("row")
    holders = lax.axis_size("col")
    if holders == 2:
        return fused(eigvec, reflectors, tfactors, offsets, owners)
    vectors, factor = reflectors[0, 0], tfactors[0, 0]
    packed = fold(factor)
    source = lax.dynamic_slice_in_dim(owners, own_row, 1, 1)[:, 0]
    begin = lax.dynamic_slice_in_dim(offsets, own_row, 1, 1)[:, 0] - (rows - WIN)
    va, vb = (from_root(vectors, "col", source[t]) for t in range(TICKS))
    ta, tb = (from_root(packed, "col", source[t]) for t in range(TICKS))
    second = jnp.arange(TICKS, dtype=jnp.int32)
    plan = jnp.stack([begin, second])
    result, head, *uppers = copy_slab(eigvec, half, width)
    lower = from_behind(head, "row", -1)
    parts, tops = [], []
    for chunk, upper in enumerate(uppers):
        part, low = apply_window(plan, va, vb, ta, tb, upper, lower, chunk)
        parts.append(part)
        tops.append(from_behind(low, "row", 1))
    result = store_upper(parts, result)
    first = (own_row == 0).astype(jnp.int32)[None]
    for chunk, top in enumerate(tops):
        result = store_top(first, top, head, result, chunk)
    return result


def solution(mesh):
    return jax.shard_map(
        per_device,
        mesh=mesh,
        in_specs=(
            P("row", "col"),
            P("row", "col", None, None),
            P("row", "col", None, None),
            P(),
            P(),
        ),
        out_specs=P("row", "col"),
        check_vma=False,
    )
```

```python
import functools

import jax
import jax.numpy as jnp
from jax import lax
from jax.experimental import pallas as pl
from jax.experimental.pallas import tpu as pltpu
from jax.sharding import PartitionSpec as P

WIN = 1024
TICKS = 2
CHUNK = 256
PAD = 8
SUB = 8
LARGE = 56
FUSED = 53
STREAMS = 8


def from_root(block, axis, owner):
    block = jnp.where(lax.axis_index(axis) == owner, block, jnp.zeros_like(block))
    return lax.psum(block, axis)


def from_behind(shard, axis, by):
    count = lax.axis_size(axis)
    pairs = [(i, i + by) for i in range(count) if 0 <= i + by < count]
    return lax.ppermute(shard, axis, pairs)


def positions(n):
    return lax.broadcasted_iota(jnp.int32, (n, n), 0), lax.broadcasted_iota(jnp.int32, (n, n), 1)


def fold(factor):
    half = factor.shape[0] // 2
    r, c = positions(half)
    first, side, second = factor[:half, :half], factor[:half, half:], factor[half:, half:]
    both = jnp.where(r <= c, first, second.T)
    diagonal = jnp.sum(jnp.where(r == c, second, 0.0), axis=0, keepdims=True)
    tail = jnp.pad(diagonal, ((0, PAD - 1), (0, half)))
    return jnp.concatenate([jnp.concatenate([both, side], 1), tail], 0)


def unfold(packed):
    half = packed.shape[1] // 2
    r, c = positions(half)
    both, side, diagonal = packed[:half, :half], packed[:half, half:], packed[half : half + 1, :half]
    first = jnp.where(r <= c, both, 0.0)
    second = jnp.where(r < c, both.T, jnp.where(r == c, jnp.broadcast_to(diagonal, both.shape), 0.0))
    return jnp.concatenate(
        [jnp.concatenate([first, side], 1), jnp.concatenate([jnp.zeros_like(first), second], 1)], 0
    )


def split(x):
    high = x.astype(jnp.bfloat16)
    return high, (x - high.astype(jnp.float32)).astype(jnp.bfloat16)


def product(left, right):
    (lh, ll), (rh, rl) = left, right
    return jnp.dot(
        jnp.concatenate([lh, lh, ll], 1),
        jnp.concatenate([rh, rl, rh], 0),
        preferred_element_type=jnp.float32,
    )


def tiles(x):
    return x.reshape(x.shape[0] // SUB, SUB, x.shape[1])


def rows_from(x, shift):
    turned = pltpu.roll(tiles(x), lax.rem(SUB - shift, SUB), axis=1)
    place = lax.broadcasted_iota(jnp.int32, turned[1:].shape, 1)
    return jnp.where(place + shift < SUB, turned[:-1], turned[1:]).reshape(x.shape[0] - SUB, x.shape[1])


def rows_at(x, shift):
    turned = pltpu.roll(tiles(x), shift, axis=1)
    none = jnp.zeros_like(turned[:1])
    ahead, behind = jnp.concatenate([turned, none], 0), jnp.concatenate([none, turned], 0)
    place = lax.broadcasted_iota(jnp.int32, ahead.shape, 1)
    return jnp.where(place >= shift, ahead, behind).reshape(x.shape[0] + SUB, x.shape[1])


def copy_kernel(width, x_ref, held, head, *uppers):
    step = x_ref.shape[0]
    at = pl.program_id(0)
    first = pl.num_programs(0) - WIN // step
    held[...] = x_ref[...]

    @pl.when(at == 0)
    def _():
        head[...] = x_ref[...]

    for part in range(WIN // step):

        @pl.when(at == first + part)
        def _():
            for chunk, upper in enumerate(uppers):
                upper[part * step : (part + 1) * step, :] = x_ref[:, chunk * width : (chunk + 1) * width]


def cost(flops, values):
    return pl.CostEstimate(flops=flops, bytes_accessed=4 * values, transcendentals=0)


def grant(mib):
    return pltpu.CompilerParams(vmem_limit_bytes=mib * 2**20)


def whole(shape):
    return pl.BlockSpec(shape, lambda i: (0,) * len(shape))


def copy_slab(eigvec, half, width):
    rows, cols = eigvec.shape
    count = cols // width
    rolling = pl.BlockSpec((half, cols), lambda i: (i, 0))
    return pl.pallas_call(
        functools.partial(copy_kernel, width),
        grid=(rows // half,),
        in_specs=[rolling],
        out_specs=[rolling, whole((half, cols))] + [whole((WIN, width))] * count,
        out_shape=[jax.ShapeDtypeStruct(eigvec.shape, jnp.float32), jax.ShapeDtypeStruct((half, cols), jnp.float32)]
        + [jax.ShapeDtypeStruct((WIN, width), jnp.float32)] * count,
        cost_estimate=cost(0, (2 * rows + half + WIN) * cols),
        compiler_params=grant(LARGE),
    )(eigvec)


def window_kernel(plan, va, vb, ta, tb, upper, lower, up_out, low_out, frame):
    end = WIN + lower.shape[0]
    frame[:WIN, :] = upper[...]
    frame[WIN:end, :] = lower[...]
    frame[end:, :] = jnp.zeros_like(frame[end:, :])
    for tick in range(TICKS):
        begin, second = plan[0, tick], plan[1, tick] > 0
        block = jnp.where(second, vb[...], va[...])
        vectors = split(block)
        factor = split(unfold(jnp.where(second, tb[...], ta[...])))
        shift = lax.rem(begin, SUB)
        near = pl.ds(pl.multiple_of(begin - shift, SUB), WIN + SUB)
        window = rows_from(frame[near, :], shift)
        coefficients = product(split(block.T), split(window))
        scaled = product(factor, split(coefficients))
        frame[near, :] -= rows_at(product(vectors, split(scaled)), shift)
    up_out[...] = frame[:WIN, :]
    low_out[...] = frame[WIN:end, :]


def apply_window(plan, va, vb, ta, tb, upper, lower, chunk):
    width = upper.shape[1]
    low = lower.shape[0]
    block = va.shape[1]
    return pl.pallas_call(
        window_kernel,
        grid=(1,),
        in_specs=[pl.BlockSpec(memory_space=pltpu.SMEM)] + [whole(x.shape) for x in (va, vb, ta, tb, upper)]
        + [pl.BlockSpec((low, width), lambda i: (0, chunk))],
        out_specs=[whole((WIN, width)), whole((low, width))],
        out_shape=[
            jax.ShapeDtypeStruct((WIN, width), jnp.float32),
            jax.ShapeDtypeStruct((low, width), jnp.float32),
        ],
        scratch_shapes=[pltpu.VMEM((WIN + low + SUB, width), jnp.float32)],
        cost_estimate=cost(3 * TICKS * 2 * width * block * (2 * WIN + block), 2 * WIN * block + 4 * WIN * width),
        compiler_params=grant(60),
    )(plan, va, vb, ta, tb, upper, lower)


def store_kernel(*refs):
    *parts, held, out = refs
    for chunk, part in enumerate(parts):
        width = part.shape[1]
        out[:, chunk * width : (chunk + 1) * width] = part[...]


def store_upper(parts, held):
    rows, cols = held.shape
    return pl.pallas_call(
        store_kernel,
        grid=(1,),
        in_specs=[whole(part.shape) for part in parts] + [pl.BlockSpec(memory_space=pltpu.HBM)],
        out_specs=pl.BlockSpec((WIN, cols), lambda i: (rows // WIN - 1, 0)),
        out_shape=jax.ShapeDtypeStruct(held.shape, jnp.float32),
        input_output_aliases={len(parts): 0},
        cost_estimate=cost(0, 2 * WIN * cols),
        compiler_params=grant(12),
    )(*parts, held)


def top_kernel(first, top, head, held, out):
    out[...] = jnp.where(first[0] > 0, head[...], top[...])


def store_top(first, top, head, held, chunk):
    half, width = top.shape
    return pl.pallas_call(
        top_kernel,
        grid=(1,),
        in_specs=[
            pl.BlockSpec(memory_space=pltpu.SMEM),
            whole(top.shape),
            pl.BlockSpec((half, width), lambda i: (0, chunk)),
            pl.BlockSpec(memory_space=pltpu.HBM),
        ],
        out_specs=pl.BlockSpec((half, width), lambda i: (0, chunk)),
        out_shape=jax.ShapeDtypeStruct(held.shape, jnp.float32),
        input_output_aliases={3: 0},
        cost_estimate=cost(0, 3 * half * width),
        compiler_params=grant(4),
    )(first, top, head, held)


PIECE = 64
PART = 256
MESH = pl.DeviceIdType.MESH


def triple(left, right):
    (lh, ll), (rh, rl) = left, right
    return jnp.dot(
        jnp.concatenate([lh, lh, ll], 1),
        jnp.concatenate([rh, rl, rh], 0),
        preferred_element_type=jnp.float32,
    )


def shifted(ref, start, count, cols):
    tile = lax.div(start, SUB)
    return rows_from(ref[pl.ds(tile * SUB, count + SUB), cols], start - tile * SUB)


def fused_kernel(
    x, v, t, offsets, owners, out, tail, tail_h, tail_l,
    frame, vectors, t_own, t_out, t_far, vt_out, vt_far, vh, vl, vth, vtl, th, tl, wh, wl, p, c, u0, u1,
    above, ah, al, ac,
    near_sem, x_sent, x_got, low_sent, low_got, y_sent, y_got,
):
    rows, cols = x.shape
    half, block = WIN // 2, v.shape[3]
    quarter = block // 2
    base = rows - WIN
    row, col = lax.axis_index("row"), lax.axis_index("col")
    last = lax.axis_size("row") - 1
    has_above, has_below = row > 0, row < last
    other, below = {"col": 1 - col}, {"row": row + 1}
    parts = [slice(at, at + PART) for at in range(0, cols, PART)]
    pieces = [slice(at, at + PIECE) for at in range(block - PIECE, -1, -PIECE)]
    count = len(pieces)
    rests = [(at, half // 2) for at in (0, half // 2)]

    def local(src, dst, which):
        return pltpu.make_async_copy(src, dst, near_sem.at[which])

    def remote(src, dst, sent, got, target):
        return pltpu.make_async_remote_copy(
            src_ref=src, dst_ref=dst, send_sem=sent, recv_sem=got, device_id=target, device_id_type=MESH
        )

    load_t = local(t.at[0, 0], t_own, 0)
    load_v = local(v.at[0, 0], vectors.at[0, pl.ds(half, WIN)], 1)
    load_upper = local(x.at[pl.ds(base, WIN)], frame.at[pl.ds(0, WIN)], 2)
    load_head = local(x.at[pl.ds(0, half)], out.at[pl.ds(0, half)], 3)
    load_middle = local(x.at[pl.ds(half, base - half)], out.at[pl.ds(half, base - half)], 4)
    send_rest = [
        remote(vectors.at[0, pl.ds(WIN + at, n)], vectors.at[1, pl.ds(WIN + at, n)], x_sent.at[k], x_got.at[k], other)
        for k, (at, n) in enumerate(rests)
    ]
    send_t = remote(t_out, t_far, x_sent.at[2], x_got.at[2], other)
    send_vt = [
        remote(vt_out.at[pl.ds(piece.start, PIECE)], vt_far.at[pl.ds(piece.start, PIECE)],
               x_sent.at[3 + k], x_got.at[3 + k], other)
        for k, piece in enumerate(pieces)
    ]
    send_low = remote(out.at[pl.ds(0, half)], frame.at[pl.ds(WIN, half)], low_sent, low_got, {"row": row - 1})
    pass_own = remote(vectors.at[0, pl.ds(WIN, half)], above.at[0, pl.ds(0, half)], y_sent.at[0], y_got.at[0], below)
    pass_far = [
        remote(vectors.at[1, pl.ds(WIN + at, n)], above.at[1, pl.ds(at, n)], y_sent.at[1 + k], y_got.at[1 + k], below)
        for k, (at, n) in enumerate(rests)
    ]
    pass_first = [
        remote(c.at[0, pl.ds(piece.start, PIECE)], ac.at[pl.ds(piece.start, PIECE)],
               y_sent.at[3 + k], y_got.at[3 + k], below)
        for k, piece in enumerate(pieces)
    ]
    pass_second = [
        remote(c.at[1, :, pl.ds(part.start, PART)], tail.at[:, pl.ds(part.start, PART)],
               y_sent.at[3 + count + k], y_got.at[3 + count + k], below)
        for k, part in enumerate(parts)
    ]

    def send_below(copy):
        @pl.when(has_below)
        def _():
            copy.start()

    load_v.start()
    load_head.start()
    load_t.start()
    barrier = pltpu.get_barrier_semaphore()
    pl.semaphore_signal(barrier, inc=1, device_id=other, device_id_type=MESH)

    @pl.when(has_above)
    def _():
        pl.semaphore_signal(barrier, inc=1, device_id={"row": row - 1}, device_id_type=MESH)

    @pl.when(has_below)
    def _():
        pl.semaphore_signal(barrier, inc=1, device_id=below, device_id_type=MESH)

    load_upper.start()

    @pl.when(has_above & has_below)
    def _():
        pl.semaphore_wait(barrier, 3)

    @pl.when(jnp.logical_not(has_above & has_below))
    def _():
        pl.semaphore_wait(barrier, 2)

    load_v.wait()
    for copy in send_rest:
        copy.start()

    load_head.wait()

    @pl.when(has_above)
    def _():
        send_low.start()

    load_middle.start()

    load_t.wait()
    factor = t_own[...]
    r, l = positions(quarter)
    first, second = factor[:quarter, :quarter], factor[quarter:, quarter:]
    diagonal = jnp.sum(jnp.where(r == l, second, 0.0), axis=0, keepdims=True)
    t_out[:quarter, :quarter] = jnp.where(r <= l, first, second.T)
    t_out[:quarter, quarter:] = factor[:quarter, quarter:]
    t_out[quarter:, :] = jnp.broadcast_to(jnp.concatenate([diagonal, diagonal], 1), (PAD, block))
    th[0], tl[0] = split(factor)

    vt_out[...] = vectors[0, half:WIN, :].T
    send_t.start()
    for copy in send_vt:
        copy.start()

    def prepare(which, start, n):
        span = slice(start, start + n)
        piece = vectors[which, half + start : half + start + n, :]
        vh[which, span, :], vl[which, span, :] = split(piece)
        vth[which, :, span], vtl[which, :, span] = split(piece.T)

    for at in range(0, WIN, half // 2):
        prepare(0, at, half // 2)

    begin = [jnp.clip(offsets[tick, row] - base, 0, half) for tick in range(TICKS)]
    holder = [(owners[tick, row] != col).astype(jnp.int32) for tick in range(TICKS)]
    before = jnp.maximum(row - 1, 0)
    above_begin = [jnp.clip(offsets[tick, before] - base, 0, half) for tick in range(TICKS)]
    above_holder = [(owners[tick, before] != col).astype(jnp.int32) for tick in range(TICKS)]
    for u in (u0, u1):
        u[:half, :] = jnp.zeros((half, cols), jnp.float32)
        u[half + WIN :, :] = jnp.zeros((half + SUB, cols), jnp.float32)
    for which in range(2):
        vectors[which, :half, :] = jnp.zeros((half, block), jnp.float32)
        vectors[which, half + WIN :, :] = jnp.zeros((half + SUB, block), jnp.float32)
        above[which, half:, :] = jnp.zeros((half + SUB, block), jnp.float32)
    frame[WIN + half :, :] = jnp.zeros((SUB, cols), jnp.float32)
    p[0] = jnp.zeros((block, cols), jnp.float32)

    @pl.when(jnp.logical_not(has_below))
    def _():
        frame[WIN : WIN + half, :] = jnp.zeros((half, cols), jnp.float32)

    for copy in send_rest:
        copy.wait_recv()
    for copy in (pass_own, *pass_far):
        send_below(copy)
    for at, n in rests:
        prepare(1, half + at, n)
    load_upper.wait()

    @pl.when(has_below)
    def _():
        send_low.wait_recv()

    def windows(k, carry):
        span = pl.ds(pl.multiple_of(k * 128, 128), 128)
        for tick in range(TICKS):
            wh[tick, span, :], wl[tick, span, :] = split(shifted(frame, begin[tick] + k * 128, 128, slice(None)))
        return carry

    lax.fori_loop(0, WIN // 128, windows, 0)

    send_t.wait_recv()
    th[1], tl[1] = split(unfold(t_far[...]))

    for k, piece in enumerate(pieces):
        send_vt[k].wait_recv()
        vth[1, piece, :half], vtl[1, piece, :half] = split(vt_far[piece, :])
        for tick in range(TICKS):
            left = vth[holder[tick], piece, :], vtl[holder[tick], piece, :]
            for part in parts:
                p[tick, piece, part] = triple(left, (wh[tick, :, part], wl[tick, :, part]))
            if tick == 0:
                left = th[holder[0], piece, :], tl[holder[0], piece, :]
                for part in parts:
                    c[0, piece, part] = triple(left, split(p[0, :, part]))
                send_below(pass_first[k])
        if piece.start % quarter == 0:
            span = slice(piece.start, piece.start + quarter)
            natural = vt_far[span, :].T
            vectors[1, half:WIN, span] = natural
            vh[1, :half, span], vl[1, :half, span] = split(natural)
        if k == 0:

            @pl.when(has_above)
            def _():
                pass_own.wait_recv()
                for copy in pass_far:
                    copy.wait_recv()
                for tick, (high, rest) in enumerate(((ah, al), (tail_h, tail_l))):
                    lower = shifted(above.at[above_holder[tick]], half - above_begin[tick], half, slice(None))
                    high[...], rest[...] = split(lower)

            @pl.when(jnp.logical_not(has_above))
            def _():
                tail[...] = jnp.zeros_like(tail)
                tail_h[...] = jnp.zeros_like(tail_h)
                tail_l[...] = jnp.zeros_like(tail_l)

    moved = split(shifted(vectors.at[holder[0]], half + begin[1] - begin[0], WIN, slice(None)))
    cross = split(triple((vth[holder[1]], vtl[holder[1]]), moved))
    factor = th[holder[1]], tl[holder[1]]
    for k, part in enumerate(parts):
        sums = p[1, :, part] - triple(cross, split(c[0, :, part]))
        c[1, :, part] = triple(factor, split(sums))
        send_below(pass_second[k])

    @pl.when(has_above)
    def _():
        send_low.wait_send()
        for copy in pass_first:
            copy.wait_recv()
        for part in parts:
            out[:half, part] -= triple((ah[...], al[...]), split(ac[:, part]))

    for part in parts:
        for tick, u in enumerate((u0, u1)):
            u[half : half + WIN, part] = triple((vh[holder[tick]], vl[holder[tick]]), split(c[tick, :, part]))

        def upper(k, carry):
            span = pl.ds(pl.multiple_of(k * 128, 128), 128)
            out[pl.ds(pl.multiple_of(base + k * 128, 128), 128), part] = (
                frame[span, part]
                - shifted(u0, half - begin[0] + k * 128, 128, part)
                - shifted(u1, half - begin[1] + k * 128, 128, part)
            )
            return carry

        lax.fori_loop(0, WIN // 128, upper, 0)

    load_middle.wait()
    for copy in (*send_rest, send_t, *send_vt):
        copy.wait_send()

    @pl.when(has_above)
    def _():
        for copy in pass_second:
            copy.wait_recv()

    @pl.when(has_below)
    def _():
        for copy in (pass_own, *pass_far, *pass_first, *pass_second):
            copy.wait_send()


def finish_kernel(held, tail, tail_h, tail_l, out, top, sems):
    rows, cols = held.shape
    half = WIN // 2
    step = (rows - half) // (STREAMS - 1)
    copies = []
    for k in range(STREAMS - 1):
        span = pl.ds(half + k * step, step)
        copies.append(pltpu.make_async_copy(held.at[span], out.at[span], sems.at[k]))
    for copy in copies:
        copy.start()
    last = pltpu.make_async_copy(top, out.at[pl.ds(0, half)], sems.at[STREAMS - 1])
    for at in range(0, cols, PART):
        part = slice(at, at + PART)
        top[:, part] = held[:half, part] - triple((tail_h[...], tail_l[...]), split(tail[:, part]))
    last.start()
    for copy in (*copies, last):
        copy.wait()


def fused(eigvec, reflectors, tfactors, offsets, owners):
    rows, cols = eigvec.shape
    block = reflectors.shape[3]
    half = WIN // 2
    count = block // PIECE
    f32, bf16 = jnp.float32, jnp.bfloat16
    dma = pltpu.SemaphoreType.DMA
    arrays = [pltpu.with_memory_space_constraint(a, pltpu.HBM) for a in (eigvec, reflectors, tfactors)]
    results = pl.pallas_call(
        fused_kernel,
        in_specs=[pl.BlockSpec(memory_space=pltpu.HBM)] * 3 + [pl.BlockSpec(memory_space=pltpu.SMEM)] * 2,
        out_specs=[pl.BlockSpec(memory_space=pltpu.VMEM)] * 4,
        out_shape=[
            pltpu.VMEM(eigvec.shape, f32),
            pltpu.VMEM((block, cols), f32),
            pltpu.VMEM((half, block), bf16),
            pltpu.VMEM((half, block), bf16),
        ],
        scratch_shapes=[
            pltpu.VMEM((WIN + half + SUB, cols), f32),
            pltpu.VMEM((2, 2 * WIN + SUB, block), f32),
            pltpu.VMEM((block, block), f32),
            pltpu.VMEM((block // 2 + PAD, block), f32),
            pltpu.VMEM((block // 2 + PAD, block), f32),
            pltpu.VMEM((block, half), f32),
            pltpu.VMEM((block, half), f32),
            pltpu.VMEM((2, WIN, block), bf16),
            pltpu.VMEM((2, WIN, block), bf16),
            pltpu.VMEM((2, block, WIN), bf16),
            pltpu.VMEM((2, block, WIN), bf16),
            pltpu.VMEM((2, block, block), bf16),
            pltpu.VMEM((2, block, block), bf16),
            pltpu.VMEM((TICKS, WIN, cols), bf16),
            pltpu.VMEM((TICKS, WIN, cols), bf16),
            pltpu.VMEM((TICKS, block, cols), f32),
            pltpu.VMEM((TICKS, block, cols), f32),
            pltpu.VMEM((2 * WIN + SUB, cols), f32),
            pltpu.VMEM((2 * WIN + SUB, cols), f32),
            pltpu.VMEM((2, WIN + SUB, block), f32),
            pltpu.VMEM((half, block), bf16),
            pltpu.VMEM((half, block), bf16),
            pltpu.VMEM((block, cols), f32),
            dma((5,)),
            dma((3 + count,)),
            dma((3 + count,)),
            dma,
            dma,
            dma((3 + count + cols // PART,)),
            dma((3 + count + cols // PART,)),
        ],
        cost_estimate=cost(10**10, 10**7),
        compiler_params=pltpu.CompilerParams(collective_id=0, has_side_effects=True, vmem_limit_bytes=FUSED * 2**20),
    )(*arrays, offsets, owners)
    return pl.pallas_call(
        finish_kernel,
        in_specs=[pl.BlockSpec(memory_space=pltpu.VMEM)] * 4,
        out_specs=pl.BlockSpec(memory_space=pltpu.HBM),
        out_shape=jax.ShapeDtypeStruct(eigvec.shape, f32),
        scratch_shapes=[pltpu.VMEM((half, cols), f32), dma((STREAMS,))],
        cost_estimate=cost(0, 2 * rows * cols),
        compiler_params=grant(8),
    )(*results)


def per_device(eigvec, reflectors, tfactors, offsets, owners):
    rows, cols = eigvec.shape
    half = WIN // 2
    width = min(CHUNK, cols)
    own_row = lax.axis_index("row")
    holders = lax.axis_size("col")
    if holders == 2:
        return fused(eigvec, reflectors, tfactors, offsets, owners)
    vectors, factor = reflectors[0, 0], tfactors[0, 0]
    packed = fold(factor)
    source = lax.dynamic_slice_in_dim(owners, own_row, 1, 1)[:, 0]
    begin = lax.dynamic_slice_in_dim(offsets, own_row, 1, 1)[:, 0] - (rows - WIN)
    va, vb = (from_root(vectors, "col", source[t]) for t in range(TICKS))
    ta, tb = (from_root(packed, "col", source[t]) for t in range(TICKS))
    second = jnp.arange(TICKS, dtype=jnp.int32)
    plan = jnp.stack([begin, second])
    result, head, *uppers = copy_slab(eigvec, half, width)
    lower = from_behind(head, "row", -1)
    parts, tops = [], []
    for chunk, upper in enumerate(uppers):
        part, low = apply_window(plan, va, vb, ta, tb, upper, lower, chunk)
        parts.append(part)
        tops.append(from_behind(low, "row", 1))
    result = store_upper(parts, result)
    first = (own_row == 0).astype(jnp.int32)[None]
    for chunk, top in enumerate(tops):
        result = store_top(first, top, head, result, chunk)
    return result


def solution(mesh):
    return jax.shard_map(
        per_device,
        mesh=mesh,
        in_specs=(
            P("row", "col"),
            P("row", "col", None, None),
            P("row", "col", None, None),
            P(),
            P(),
        ),
        out_specs=P("row", "col"),
        check_vma=False,
    )
```

```python
import functools

import jax
import jax.numpy as jnp
from jax import lax
from jax.experimental import pallas as pl
from jax.experimental.pallas import tpu as pltpu
from jax.sharding import PartitionSpec as P

WIN = 1024
TICKS = 2
CHUNK = 256
PAD = 8
SUB = 8
LARGE = 56
FUSED = 53
STREAMS = 8


def from_root(block, axis, owner):
    block = jnp.where(lax.axis_index(axis) == owner, block, jnp.zeros_like(block))
    return lax.psum(block, axis)


def from_behind(shard, axis, by):
    count = lax.axis_size(axis)
    pairs = [(i, i + by) for i in range(count) if 0 <= i + by < count]
    return lax.ppermute(shard, axis, pairs)


def positions(n):
    return lax.broadcasted_iota(jnp.int32, (n, n), 0), lax.broadcasted_iota(jnp.int32, (n, n), 1)


def fold(factor):
    half = factor.shape[0] // 2
    r, c = positions(half)
    first, side, second = factor[:half, :half], factor[:half, half:], factor[half:, half:]
    both = jnp.where(r <= c, first, second.T)
    diagonal = jnp.sum(jnp.where(r == c, second, 0.0), axis=0, keepdims=True)
    tail = jnp.pad(diagonal, ((0, PAD - 1), (0, half)))
    return jnp.concatenate([jnp.concatenate([both, side], 1), tail], 0)


def unfold(packed):
    half = packed.shape[1] // 2
    r, c = positions(half)
    both, side, diagonal = packed[:half, :half], packed[:half, half:], packed[half : half + 1, :half]
    first = jnp.where(r <= c, both, 0.0)
    second = jnp.where(r < c, both.T, jnp.where(r == c, jnp.broadcast_to(diagonal, both.shape), 0.0))
    return jnp.concatenate(
        [jnp.concatenate([first, side], 1), jnp.concatenate([jnp.zeros_like(first), second], 1)], 0
    )


def split(x):
    high = x.astype(jnp.bfloat16)
    return high, (x - high.astype(jnp.float32)).astype(jnp.bfloat16)


def product(left, right):
    (lh, ll), (rh, rl) = left, right
    return jnp.dot(
        jnp.concatenate([lh, lh, ll], 1),
        jnp.concatenate([rh, rl, rh], 0),
        preferred_element_type=jnp.float32,
    )


def tiles(x):
    return x.reshape(x.shape[0] // SUB, SUB, x.shape[1])


def rows_from(x, shift):
    turned = pltpu.roll(tiles(x), lax.rem(SUB - shift, SUB), axis=1)
    place = lax.broadcasted_iota(jnp.int32, turned[1:].shape, 1)
    return jnp.where(place + shift < SUB, turned[:-1], turned[1:]).reshape(x.shape[0] - SUB, x.shape[1])


def rows_at(x, shift):
    turned = pltpu.roll(tiles(x), shift, axis=1)
    none = jnp.zeros_like(turned[:1])
    ahead, behind = jnp.concatenate([turned, none], 0), jnp.concatenate([none, turned], 0)
    place = lax.broadcasted_iota(jnp.int32, ahead.shape, 1)
    return jnp.where(place >= shift, ahead, behind).reshape(x.shape[0] + SUB, x.shape[1])


def copy_kernel(width, x_ref, held, head, *uppers):
    step = x_ref.shape[0]
    at = pl.program_id(0)
    first = pl.num_programs(0) - WIN // step
    held[...] = x_ref[...]

    @pl.when(at == 0)
    def _():
        head[...] = x_ref[...]

    for part in range(WIN // step):

        @pl.when(at == first + part)
        def _():
            for chunk, upper in enumerate(uppers):
                upper[part * step : (part + 1) * step, :] = x_ref[:, chunk * width : (chunk + 1) * width]


def cost(flops, values):
    return pl.CostEstimate(flops=flops, bytes_accessed=4 * values, transcendentals=0)


def grant(mib):
    return pltpu.CompilerParams(vmem_limit_bytes=mib * 2**20)


def whole(shape):
    return pl.BlockSpec(shape, lambda i: (0,) * len(shape))


def copy_slab(eigvec, half, width):
    rows, cols = eigvec.shape
    count = cols // width
    rolling = pl.BlockSpec((half, cols), lambda i: (i, 0))
    return pl.pallas_call(
        functools.partial(copy_kernel, width),
        grid=(rows // half,),
        in_specs=[rolling],
        out_specs=[rolling, whole((half, cols))] + [whole((WIN, width))] * count,
        out_shape=[jax.ShapeDtypeStruct(eigvec.shape, jnp.float32), jax.ShapeDtypeStruct((half, cols), jnp.float32)]
        + [jax.ShapeDtypeStruct((WIN, width), jnp.float32)] * count,
        cost_estimate=cost(0, (2 * rows + half + WIN) * cols),
        compiler_params=grant(LARGE),
    )(eigvec)


def window_kernel(plan, va, vb, ta, tb, upper, lower, up_out, low_out, frame):
    end = WIN + lower.shape[0]
    frame[:WIN, :] = upper[...]
    frame[WIN:end, :] = lower[...]
    frame[end:, :] = jnp.zeros_like(frame[end:, :])
    for tick in range(TICKS):
        begin, second = plan[0, tick], plan[1, tick] > 0
        block = jnp.where(second, vb[...], va[...])
        vectors = split(block)
        factor = split(unfold(jnp.where(second, tb[...], ta[...])))
        shift = lax.rem(begin, SUB)
        near = pl.ds(pl.multiple_of(begin - shift, SUB), WIN + SUB)
        window = rows_from(frame[near, :], shift)
        coefficients = product(split(block.T), split(window))
        scaled = product(factor, split(coefficients))
        frame[near, :] -= rows_at(product(vectors, split(scaled)), shift)
    up_out[...] = frame[:WIN, :]
    low_out[...] = frame[WIN:end, :]


def apply_window(plan, va, vb, ta, tb, upper, lower, chunk):
    width = upper.shape[1]
    low = lower.shape[0]
    block = va.shape[1]
    return pl.pallas_call(
        window_kernel,
        grid=(1,),
        in_specs=[pl.BlockSpec(memory_space=pltpu.SMEM)] + [whole(x.shape) for x in (va, vb, ta, tb, upper)]
        + [pl.BlockSpec((low, width), lambda i: (0, chunk))],
        out_specs=[whole((WIN, width)), whole((low, width))],
        out_shape=[
            jax.ShapeDtypeStruct((WIN, width), jnp.float32),
            jax.ShapeDtypeStruct((low, width), jnp.float32),
        ],
        scratch_shapes=[pltpu.VMEM((WIN + low + SUB, width), jnp.float32)],
        cost_estimate=cost(3 * TICKS * 2 * width * block * (2 * WIN + block), 2 * WIN * block + 4 * WIN * width),
        compiler_params=grant(60),
    )(plan, va, vb, ta, tb, upper, lower)


def store_kernel(*refs):
    *parts, held, out = refs
    for chunk, part in enumerate(parts):
        width = part.shape[1]
        out[:, chunk * width : (chunk + 1) * width] = part[...]


def store_upper(parts, held):
    rows, cols = held.shape
    return pl.pallas_call(
        store_kernel,
        grid=(1,),
        in_specs=[whole(part.shape) for part in parts] + [pl.BlockSpec(memory_space=pltpu.HBM)],
        out_specs=pl.BlockSpec((WIN, cols), lambda i: (rows // WIN - 1, 0)),
        out_shape=jax.ShapeDtypeStruct(held.shape, jnp.float32),
        input_output_aliases={len(parts): 0},
        cost_estimate=cost(0, 2 * WIN * cols),
        compiler_params=grant(12),
    )(*parts, held)


def top_kernel(first, top, head, held, out):
    out[...] = jnp.where(first[0] > 0, head[...], top[...])


def store_top(first, top, head, held, chunk):
    half, width = top.shape
    return pl.pallas_call(
        top_kernel,
        grid=(1,),
        in_specs=[
            pl.BlockSpec(memory_space=pltpu.SMEM),
            whole(top.shape),
            pl.BlockSpec((half, width), lambda i: (0, chunk)),
            pl.BlockSpec(memory_space=pltpu.HBM),
        ],
        out_specs=pl.BlockSpec((half, width), lambda i: (0, chunk)),
        out_shape=jax.ShapeDtypeStruct(held.shape, jnp.float32),
        input_output_aliases={3: 0},
        cost_estimate=cost(0, 3 * half * width),
        compiler_params=grant(4),
    )(first, top, head, held)


PIECE = 64
PART = 256
MESH = pl.DeviceIdType.MESH


def triple(left, right):
    (lh, ll), (rh, rl) = left, right
    return jnp.dot(
        jnp.concatenate([lh, lh, ll], 1),
        jnp.concatenate([rh, rl, rh], 0),
        preferred_element_type=jnp.float32,
    )


def thin(left, right):
    (lh, ll), (rh, rl) = left, right
    count = lh.shape[0]
    both = jnp.dot(jnp.concatenate([lh, ll], 0), rh, preferred_element_type=jnp.float32)
    return both[:count] + (both[count:] + jnp.dot(lh, rl, preferred_element_type=jnp.float32))


def shifted(ref, start, count, cols):
    tile = lax.div(start, SUB)
    return rows_from(ref[pl.ds(tile * SUB, count + SUB), cols], start - tile * SUB)


def fused_kernel(
    x, v, t, offsets, owners, out, tail, tail_h, tail_l,
    frame, vectors, t_own, t_out, t_far, vt_out, vt_far, vh, vl, vth, vtl, th, tl, wh, wl, p, c, u0, u1,
    above, ah, al, ac, mh, ml, ph, pl_, ch, cl,
    near_sem, x_sent, x_got, low_sent, low_got, y_sent, y_got,
):
    rows, cols = x.shape
    half, block = WIN // 2, v.shape[3]
    quarter = block // 2
    base = rows - WIN
    row, col = lax.axis_index("row"), lax.axis_index("col")
    last = lax.axis_size("row") - 1
    has_above, has_below = row > 0, row < last
    other, below = {"col": 1 - col}, {"row": row + 1}
    parts = [slice(at, at + PART) for at in range(0, cols, PART)]
    pieces = [slice(at, at + PIECE) for at in range(block - PIECE, -1, -PIECE)]
    count = len(pieces)
    rests = [(at, half // 2) for at in (0, half // 2)]

    def local(src, dst, which):
        return pltpu.make_async_copy(src, dst, near_sem.at[which])

    def remote(src, dst, sent, got, target):
        return pltpu.make_async_remote_copy(
            src_ref=src, dst_ref=dst, send_sem=sent, recv_sem=got, device_id=target, device_id_type=MESH
        )

    load_t = local(t.at[0, 0], t_own, 0)
    load_v = local(v.at[0, 0], vectors.at[0, pl.ds(half, WIN)], 1)
    load_upper = local(x.at[pl.ds(base, WIN)], frame.at[pl.ds(0, WIN)], 2)
    load_head = local(x.at[pl.ds(0, half)], out.at[pl.ds(0, half)], 3)
    load_middle = local(x.at[pl.ds(half, base - half)], out.at[pl.ds(half, base - half)], 4)
    send_rest = [
        remote(vectors.at[0, pl.ds(WIN + at, n)], vectors.at[1, pl.ds(WIN + at, n)], x_sent.at[k], x_got.at[k], other)
        for k, (at, n) in enumerate(rests)
    ]
    send_t = remote(t_out, t_far, x_sent.at[2], x_got.at[2], other)
    send_vt = [
        remote(vt_out.at[pl.ds(piece.start, PIECE)], vt_far.at[pl.ds(piece.start, PIECE)],
               x_sent.at[3 + k], x_got.at[3 + k], other)
        for k, piece in enumerate(pieces)
    ]
    send_low = remote(out.at[pl.ds(0, half)], frame.at[pl.ds(WIN, half)], low_sent, low_got, {"row": row - 1})
    pass_own = remote(vectors.at[0, pl.ds(WIN, half)], above.at[0, pl.ds(0, half)], y_sent.at[0], y_got.at[0], below)
    pass_far = [
        remote(vectors.at[1, pl.ds(WIN + at, n)], above.at[1, pl.ds(at, n)], y_sent.at[1 + k], y_got.at[1 + k], below)
        for k, (at, n) in enumerate(rests)
    ]
    pass_first = [
        remote(c.at[0, pl.ds(piece.start, PIECE)], ac.at[pl.ds(piece.start, PIECE)],
               y_sent.at[3 + k], y_got.at[3 + k], below)
        for k, piece in enumerate(pieces)
    ]
    pass_second = [
        remote(c.at[1, :, pl.ds(part.start, PART)], tail.at[:, pl.ds(part.start, PART)],
               y_sent.at[3 + count + k], y_got.at[3 + count + k], below)
        for k, part in enumerate(parts)
    ]

    def send_below(copy):
        @pl.when(has_below)
        def _():
            copy.start()

    load_head.start()
    load_v.start()
    load_t.start()
    barrier = pltpu.get_barrier_semaphore()
    pl.semaphore_signal(barrier, inc=1, device_id=other, device_id_type=MESH)

    @pl.when(has_above)
    def _():
        pl.semaphore_signal(barrier, inc=1, device_id={"row": row - 1}, device_id_type=MESH)

    @pl.when(has_below)
    def _():
        pl.semaphore_signal(barrier, inc=1, device_id=below, device_id_type=MESH)

    load_upper.start()

    @pl.when(has_above & has_below)
    def _():
        pl.semaphore_wait(barrier, 3)

    @pl.when(jnp.logical_not(has_above & has_below))
    def _():
        pl.semaphore_wait(barrier, 2)

    load_head.wait()

    @pl.when(has_above)
    def _():
        send_low.start()

    load_v.wait()
    for copy in send_rest:
        copy.start()

    load_middle.start()

    load_t.wait()
    factor = t_own[...]
    r, l = positions(quarter)
    first, second = factor[:quarter, :quarter], factor[quarter:, quarter:]
    diagonal = jnp.sum(jnp.where(r == l, second, 0.0), axis=0, keepdims=True)
    t_out[:quarter, :quarter] = jnp.where(r <= l, first, second.T)
    t_out[:quarter, quarter:] = factor[:quarter, quarter:]
    t_out[quarter:, :] = jnp.broadcast_to(jnp.concatenate([diagonal, diagonal], 1), (PAD, block))
    th[0], tl[0] = split(factor)

    vt_out[...] = vectors[0, half:WIN, :].T
    send_t.start()
    for copy in send_vt:
        copy.start()

    def prepare(which, start, n):
        span = slice(start, start + n)
        piece = vectors[which, half + start : half + start + n, :]
        vh[which, span, :], vl[which, span, :] = split(piece)
        vth[which, :, span], vtl[which, :, span] = split(piece.T)

    for at in range(0, WIN, half // 2):
        prepare(0, at, half // 2)

    begin = [jnp.clip(offsets[tick, row] - base, 0, half) for tick in range(TICKS)]
    holder = [(owners[tick, row] != col).astype(jnp.int32) for tick in range(TICKS)]
    before = jnp.maximum(row - 1, 0)
    above_begin = [jnp.clip(offsets[tick, before] - base, 0, half) for tick in range(TICKS)]
    above_holder = [(owners[tick, before] != col).astype(jnp.int32) for tick in range(TICKS)]
    for u in (u0, u1):
        u[:half, :] = jnp.zeros((half, cols), jnp.float32)
        u[half + WIN :, :] = jnp.zeros((half + SUB, cols), jnp.float32)
    for which in range(2):
        vectors[which, :half, :] = jnp.zeros((half, block), jnp.float32)
        vectors[which, half + WIN :, :] = jnp.zeros((half + SUB, block), jnp.float32)
        above[which, half:, :] = jnp.zeros((half + SUB, block), jnp.float32)
    frame[WIN + half :, :] = jnp.zeros((SUB, cols), jnp.float32)
    ph[...] = jnp.zeros_like(ph)
    pl_[...] = jnp.zeros_like(pl_)

    @pl.when(jnp.logical_not(has_below))
    def _():
        frame[WIN : WIN + half, :] = jnp.zeros((half, cols), jnp.float32)

    for copy in send_rest:
        copy.wait_recv()
    for copy in (pass_own, *pass_far):
        send_below(copy)
    for at, n in rests:
        prepare(1, half + at, n)
    load_upper.wait()

    @pl.when(has_below)
    def _():
        send_low.wait_recv()

    def windows(k, carry):
        span = pl.ds(pl.multiple_of(k * 128, 128), 128)
        for tick in range(TICKS):
            wh[tick, span, :], wl[tick, span, :] = split(shifted(frame, begin[tick] + k * 128, 128, slice(None)))
        return carry

    lax.fori_loop(0, WIN // 128, windows, 0)

    send_t.wait_recv()
    th[1], tl[1] = split(unfold(t_far[...]))

    for k, piece in enumerate(pieces):
        send_vt[k].wait_recv()
        vth[1, piece, :half], vtl[1, piece, :half] = split(vt_far[piece, :])
        for tick in range(TICKS):
            left = vth[holder[tick], piece, :], vtl[holder[tick], piece, :]
            for part in parts:
                sums = thin(left, (wh[tick, :, part], wl[tick, :, part]))
                if tick == 0:
                    ph[piece, part], pl_[piece, part] = split(sums)
                else:
                    p[piece, part] = sums
            if tick == 0:
                left = th[holder[0], piece, :], tl[holder[0], piece, :]
                for part in parts:
                    scaled = thin(left, (ph[:, part], pl_[:, part]))
                    c[0, piece, part] = scaled
                    ch[piece, part], cl[piece, part] = split(scaled)
                send_below(pass_first[k])
        if piece.start % quarter == 0:
            span = slice(piece.start, piece.start + quarter)
            natural = vt_far[span, :].T
            vectors[1, half:WIN, span] = natural
            vh[1, :half, span], vl[1, :half, span] = split(natural)
            moved = shifted(vectors.at[holder[0]], half + begin[1] - begin[0], WIN, span)
            mh[:, span], ml[:, span] = split(moved)
        if k == 0:

            @pl.when(has_above)
            def _():
                pass_own.wait_recv()
                for copy in pass_far:
                    copy.wait_recv()
                for tick, (high, rest) in enumerate(((ah, al), (tail_h, tail_l))):
                    lower = shifted(above.at[above_holder[tick]], half - above_begin[tick], half, slice(None))
                    high[...], rest[...] = split(lower)

            @pl.when(jnp.logical_not(has_above))
            def _():
                tail[...] = jnp.zeros_like(tail)
                tail_h[...] = jnp.zeros_like(tail_h)
                tail_l[...] = jnp.zeros_like(tail_l)

    cross = split(triple((vth[holder[1]], vtl[holder[1]]), (mh[...], ml[...])))
    factor = th[holder[1]], tl[holder[1]]
    for k, part in enumerate(parts):
        sums = p[:, part] - triple(cross, (ch[:, part], cl[:, part]))
        c[1, :, part] = triple(factor, split(sums))
        send_below(pass_second[k])

    @pl.when(has_above)
    def _():
        send_low.wait_send()
        for copy in pass_first:
            copy.wait_recv()
        for part in parts:
            out[:half, part] -= triple((ah[...], al[...]), split(ac[:, part]))

    for part in parts:
        for tick, u in enumerate((u0, u1)):
            u[half : half + WIN, part] = triple((vh[holder[tick]], vl[holder[tick]]), split(c[tick, :, part]))

        def upper(k, carry):
            span = pl.ds(pl.multiple_of(k * 128, 128), 128)
            out[pl.ds(pl.multiple_of(base + k * 128, 128), 128), part] = (
                frame[span, part]
                - shifted(u0, half - begin[0] + k * 128, 128, part)
                - shifted(u1, half - begin[1] + k * 128, 128, part)
            )
            return carry

        lax.fori_loop(0, WIN // 128, upper, 0)

    load_middle.wait()
    for copy in (*send_rest, send_t, *send_vt):
        copy.wait_send()

    @pl.when(has_above)
    def _():
        for copy in pass_second:
            copy.wait_recv()

    @pl.when(has_below)
    def _():
        for copy in (pass_own, *pass_far, *pass_first, *pass_second):
            copy.wait_send()


def finish_kernel(held, tail, tail_h, tail_l, out, top, sems):
    rows, cols = held.shape
    half = WIN // 2
    step = (rows - half) // (STREAMS - 1)
    copies = []
    for k in range(STREAMS - 1):
        span = pl.ds(half + k * step, step)
        copies.append(pltpu.make_async_copy(held.at[span], out.at[span], sems.at[k]))
    for copy in copies:
        copy.start()
    last = pltpu.make_async_copy(top, out.at[pl.ds(0, half)], sems.at[STREAMS - 1])
    for at in range(0, cols, PART):
        part = slice(at, at + PART)
        top[:, part] = held[:half, part] - triple((tail_h[...], tail_l[...]), split(tail[:, part]))
    last.start()
    for copy in (*copies, last):
        copy.wait()


def fused(eigvec, reflectors, tfactors, offsets, owners):
    rows, cols = eigvec.shape
    block = reflectors.shape[3]
    half = WIN // 2
    count = block // PIECE
    f32, bf16 = jnp.float32, jnp.bfloat16
    dma = pltpu.SemaphoreType.DMA
    arrays = [pltpu.with_memory_space_constraint(a, pltpu.HBM) for a in (eigvec, reflectors, tfactors)]
    results = pl.pallas_call(
        fused_kernel,
        in_specs=[pl.BlockSpec(memory_space=pltpu.HBM)] * 3 + [pl.BlockSpec(memory_space=pltpu.SMEM)] * 2,
        out_specs=[pl.BlockSpec(memory_space=pltpu.VMEM)] * 4,
        out_shape=[
            pltpu.VMEM(eigvec.shape, f32),
            pltpu.VMEM((block, cols), f32),
            pltpu.VMEM((half, block), bf16),
            pltpu.VMEM((half, block), bf16),
        ],
        scratch_shapes=[
            pltpu.VMEM((WIN + half + SUB, cols), f32),
            pltpu.VMEM((2, 2 * WIN + SUB, block), f32),
            pltpu.VMEM((block, block), f32),
            pltpu.VMEM((block // 2 + PAD, block), f32),
            pltpu.VMEM((block // 2 + PAD, block), f32),
            pltpu.VMEM((block, half), f32),
            pltpu.VMEM((block, half), f32),
            pltpu.VMEM((2, WIN, block), bf16),
            pltpu.VMEM((2, WIN, block), bf16),
            pltpu.VMEM((2, block, WIN), bf16),
            pltpu.VMEM((2, block, WIN), bf16),
            pltpu.VMEM((2, block, block), bf16),
            pltpu.VMEM((2, block, block), bf16),
            pltpu.VMEM((TICKS, WIN, cols), bf16),
            pltpu.VMEM((TICKS, WIN, cols), bf16),
            pltpu.VMEM((block, cols), f32),
            pltpu.VMEM((TICKS, block, cols), f32),
            pltpu.VMEM((2 * WIN + SUB, cols), f32),
            pltpu.VMEM((2 * WIN + SUB, cols), f32),
            pltpu.VMEM((2, WIN + SUB, block), f32),
            pltpu.VMEM((half, block), bf16),
            pltpu.VMEM((half, block), bf16),
            pltpu.VMEM((block, cols), f32),
            pltpu.VMEM((WIN, block), bf16),
            pltpu.VMEM((WIN, block), bf16),
            pltpu.VMEM((block, cols), bf16),
            pltpu.VMEM((block, cols), bf16),
            pltpu.VMEM((block, cols), bf16),
            pltpu.VMEM((block, cols), bf16),
            dma((5,)),
            dma((3 + count,)),
            dma((3 + count,)),
            dma,
            dma,
            dma((3 + count + cols // PART,)),
            dma((3 + count + cols // PART,)),
        ],
        cost_estimate=cost(10**10, 10**7),
        compiler_params=pltpu.CompilerParams(collective_id=0, has_side_effects=True, vmem_limit_bytes=FUSED * 2**20),
    )(*arrays, offsets, owners)
    return pl.pallas_call(
        finish_kernel,
        in_specs=[pl.BlockSpec(memory_space=pltpu.VMEM)] * 4,
        out_specs=pl.BlockSpec(memory_space=pltpu.HBM),
        out_shape=jax.ShapeDtypeStruct(eigvec.shape, f32),
        scratch_shapes=[pltpu.VMEM((half, cols), f32), dma((STREAMS,))],
        cost_estimate=cost(0, 2 * rows * cols),
        compiler_params=grant(8),
    )(*results)


def per_device(eigvec, reflectors, tfactors, offsets, owners):
    rows, cols = eigvec.shape
    half = WIN // 2
    width = min(CHUNK, cols)
    own_row = lax.axis_index("row")
    holders = lax.axis_size("col")
    if holders == 2:
        return fused(eigvec, reflectors, tfactors, offsets, owners)
    vectors, factor = reflectors[0, 0], tfactors[0, 0]
    packed = fold(factor)
    source = lax.dynamic_slice_in_dim(owners, own_row, 1, 1)[:, 0]
    begin = lax.dynamic_slice_in_dim(offsets, own_row, 1, 1)[:, 0] - (rows - WIN)
    va, vb = (from_root(vectors, "col", source[t]) for t in range(TICKS))
    ta, tb = (from_root(packed, "col", source[t]) for t in range(TICKS))
    second = jnp.arange(TICKS, dtype=jnp.int32)
    plan = jnp.stack([begin, second])
    result, head, *uppers = copy_slab(eigvec, half, width)
    lower = from_behind(head, "row", -1)
    parts, tops = [], []
    for chunk, upper in enumerate(uppers):
        part, low = apply_window(plan, va, vb, ta, tb, upper, lower, chunk)
        parts.append(part)
        tops.append(from_behind(low, "row", 1))
    result = store_upper(parts, result)
    first = (own_row == 0).astype(jnp.int32)[None]
    for chunk, top in enumerate(tops):
        result = store_top(first, top, head, result, chunk)
    return result


def solution(mesh):
    return jax.shard_map(
        per_device,
        mesh=mesh,
        in_specs=(
            P("row", "col"),
            P("row", "col", None, None),
            P("row", "col", None, None),
            P(),
            P(),
        ),
        out_specs=P("row", "col"),
        check_vma=False,
    )
```
